32 devices in a mesh: group: 4 (over y, x), expert: 4 (over z), dp: 2 (over core).
Axes of the slice: x: 2, y: 2, z: 4, core: 2. Of those that a mesh axis runs over, the one named last changes fastest.
Arguments:
- tokens: bfloat16 [8, 16, 7168], P(('expert', 'dp'), 'group'), may hold values from -6 to 6
- expert_ids: int32 [8, 16, 8], P(('expert', 'dp')), may hold values from 0 to 31, as said below
- gate_codes: int32 [8, 16, 8], P(('expert', 'dp')), may hold values from 1 to 1023
- w_gate: bfloat16 [4, 7168, 2048], P('expert', None, 'group'), may hold values from -0.0625 to 0.0625
- w_up: bfloat16 [4, 7168, 2048], P('expert', None, 'group'), may hold values from -0.0625 to 0.0625
- w_down: bfloat16 [4, 2048, 7168], P('expert', 'group'), may hold values from -0.125 to 0.125
Outputs:
- mixed: bfloat16 [8, 16, 7168], P(('expert', 'dp'), 'group')
The draws below stay inside these ranges and needn't reach their ends.
Inputs may be any that keep to these rules, and one draw needn't show every extreme that they name: `expert_ids`: each token names 8 different experts, all within at most 4 of the 8 groups of 4 consecutive ids. In every set (one index of the first dimension), each expert below 4 is named by at most 4 tokens, and some expert by exactly 4; a token names at most 4 experts below 4.
All inputs are finite; a program needn't handle non-finite values.
Results may differ from the reference program's by a relative error of at most 0.015.
Values may be sent and summed in bfloat16 or wider, within the bound.
A program may use at most 64 MiB of HBM per device.

```python
import jax
import jax.numpy as jnp
from jax import lax

D = 7168
FF = 2048
TOP = 8
NODE_GROUPS = 8
MAX_NODES = 4
CAPG = 4
EXPERTS = 4
SET_TOK = 16
SETS = 8
N_GROUP = 4


def draw_others(key, count):
    keys = jax.random.split(key, 3)
    groups = jax.random.permutation(keys[0], NODE_GROUPS - 1)[:MAX_NODES] + 1
    fewer = jax.random.permutation(keys[1], (MAX_NODES - 1) * EXPERTS)[:TOP]
    wider = jax.random.permutation(keys[2], MAX_NODES * EXPERTS)[:TOP]
    local = jnp.where(count > 0, fewer, wider)
    return groups[local // EXPERTS] * EXPERTS + local % EXPERTS


def shuffle_row(key, row):
    return jax.random.permutation(key, row)


def draw_one_set(key):
    keys = jax.random.split(key, 6)
    spacing = SET_TOK // CAPG
    offsets = jax.random.permutation(keys[0], SET_TOK)[:EXPERTS]
    order = jax.random.permutation(keys[1], SET_TOK)
    slot_index = jnp.arange(CAPG)
    slot_token = order[(offsets[:, None] + spacing * slot_index[None, :]) % SET_TOK]
    live = jax.random.randint(keys[2], (EXPERTS, CAPG), 0, 2)
    chosen = jax.random.randint(keys[3], (), 0, EXPERTS)
    live = jnp.where(jnp.arange(EXPERTS)[:, None] == chosen, 1, live)
    token_index = jnp.arange(SET_TOK)
    member = jnp.sum(jnp.where(slot_token[None, :, :] == token_index[:, None, None], live[None, :, :], 0), axis=2)
    count = jnp.sum(member, axis=1)
    position = jnp.cumsum(member, axis=1) - member
    picks = jnp.arange(TOP)
    window_ids = jnp.sum(jnp.where((member[:, :, None] == 1) & (position[:, :, None] == picks[None, None, :]), jnp.arange(EXPERTS)[None, :, None], 0), axis=1)
    others = jax.vmap(draw_others)(jax.random.split(keys[4], SET_TOK), count)
    offset_pick = jnp.clip(picks[None, :] - count[:, None], 0, TOP - 1)
    other_ids = jnp.take_along_axis(others, offset_pick, axis=1)
    chosen_ids = jnp.where(picks[None, :] < count[:, None], window_ids, other_ids)
    return jax.vmap(shuffle_row)(jax.random.split(keys[5], SET_TOK), chosen_ids)


def draw_expert_ids(key, part):
    keys = jax.random.split(jax.random.fold_in(key, 17), SETS)
    return jax.vmap(draw_one_set)(keys).astype(jnp.int32)


def with_ends(array, key, low, high):
    index_at = [jax.random.randint(jax.random.fold_in(key, axis), (), 0, length) for axis, length in enumerate(array.shape)]
    longest = array.shape.index(max(array.shape))
    beside = index_at[:longest] + [(index_at[longest] + 1) % array.shape[longest]] + index_at[longest + 1:]
    return array.at[tuple(index_at)].set(low).at[tuple(beside)].set(high)


def block_levels(key, shape, pieces, smallest, largest):
    def one(axis_at, blocks):
        steps = jax.random.uniform(jax.random.fold_in(jax.random.fold_in(key, 6), axis_at), (blocks,), jnp.float32, smallest / len(pieces), largest / len(pieces))
        return jnp.repeat(jnp.exp(steps), shape[axis_at] // blocks).reshape((-1,) + (1,) * (len(shape) - axis_at - 1))

    level = one(*pieces[0])
    for cut in pieces[1:]:
        level = level * one(*cut)
    return level


def noise(rng, dims, deviation, bound, shards=(), kind=jnp.bfloat16):
    array = deviation * jax.random.normal(rng, dims, jnp.float32)
    if shards:
        array = array * block_levels(rng, dims, shards, -0.22, 0.18)
    return jnp.clip(array, -bound, bound).astype(kind)


def setup_inputs(seed: int = 0) -> dict:
    key_of = jax.random.split(jax.random.key(seed), 7)
    return {
        "tokens": noise(key_of[0], (SETS, SET_TOK, D), 1.0, 6.0, ((0, 8), (1, 4))),
        "expert_ids": draw_expert_ids(jax.random.fold_in(key_of[6], 71), 0),
        "gate_codes": with_ends(jax.random.randint(key_of[2], (SETS, SET_TOK, TOP), 1, 1024), jax.random.fold_in(key_of[2], 1), 1, 1023).astype(jnp.int32),
        "w_gate": noise(key_of[3], (EXPERTS, D, FF), D ** -0.5, 0.0625, ((0, 4), (2, 4))),
        "w_up": noise(key_of[4], (EXPERTS, D, FF), D ** -0.5, 0.0625, ((0, 4), (2, 4))),
        "w_down": noise(key_of[5], (EXPERTS, FF, D), FF ** -0.5, 0.125, ((0, 4), (1, 4))),
    }


def routing(expert_ids, gate_codes):
    codes = gate_codes.astype(jnp.float32)
    gates = 2.5 * codes / jnp.sum(codes, axis=-1, keepdims=True)
    window = jnp.arange(EXPERTS, dtype=jnp.int32)
    hits = expert_ids[..., None] == window
    member = jnp.any(hits, axis=-2).astype(jnp.int32)
    weight = jnp.sum(jnp.where(hits, gates[..., None], jnp.float32(0.0)), axis=-2)
    rank = jnp.cumsum(member, axis=-2) - member
    slots = jnp.arange(CAPG, dtype=jnp.int32)
    place = (member[..., None] == 1) & (rank[..., None] == slots)
    return place, weight


def reference(tokens, expert_ids, gate_codes, w_gate, w_up, w_down):
    place, weight = routing(expert_ids, gate_codes)
    pick = place.astype(jnp.float32)
    rows = jnp.einsum("stej,std->sejd", pick, tokens.astype(jnp.float32)).astype(jnp.bfloat16)
    slices = N_GROUP
    hid_dev = FF // slices

    def one_expert(items):
        expert_rows, gate_mat, up_mat, down_mat = items
        flat = expert_rows.reshape(SETS * CAPG, D)
        first = jnp.dot(flat, gate_mat, preferred_element_type=jnp.float32)
        second = jnp.dot(flat, up_mat, preferred_element_type=jnp.float32)
        hidden = (jax.nn.silu(first) * second).astype(jnp.bfloat16)
        parts = jnp.einsum("rgh,ghd->grd", hidden.reshape(SETS * CAPG, slices, hid_dev).astype(jnp.float32),
                           down_mat.reshape(slices, hid_dev, D).astype(jnp.float32))
        parts = lax.optimization_barrier(parts.astype(jnp.bfloat16)).astype(jnp.float32)
        return jnp.sum(parts, axis=0).reshape(SETS, CAPG, D)

    outs = lax.map(one_expert, (jnp.transpose(rows, (1, 0, 2, 3)), w_gate, w_up, w_down))
    mix = jnp.where(place, weight[..., None], jnp.float32(0.0))
    mixed = jnp.einsum("stej,esjd->std", mix, outs, precision=lax.Precision.HIGHEST)
    return mixed.astype(jnp.bfloat16)
```

```python
import functools

import jax
import jax.numpy as jnp
from jax import lax
from jax.experimental import pallas as pl
from jax.experimental.pallas import tpu as pltpu
from jax.sharding import PartitionSpec as P

CAPG = 4
CHUNKS = 4
MESH = pl.DeviceIdType.MESH


def dot(a, b):
    return jnp.dot(a, b, preferred_element_type=jnp.float32)


def routing(ids, codes, experts, capacity):
    tokens = ids.shape[0]
    wide = experts * capacity
    codes = codes.astype(jnp.float32)
    gates = 2.5 * codes / jnp.sum(codes, axis=-1, keepdims=True)
    lane = lax.broadcasted_iota(jnp.int32, (tokens, wide), 1)
    member = jnp.zeros((tokens, wide), jnp.float32)
    weight = jnp.zeros((tokens, wide), jnp.float32)
    for e in range(experts):
        hits = ids == e
        named = jnp.max(jnp.where(hits, 1.0, 0.0), axis=-1, keepdims=True)
        gate = jnp.sum(jnp.where(hits, gates, 0.0), axis=-1, keepdims=True)
        mine = (lane >= e * capacity) & (lane < (e + 1) * capacity)
        member = jnp.where(mine, named, member)
        weight = jnp.where(mine, gate, weight)
    row = lax.broadcasted_iota(jnp.int32, (tokens, tokens), 0)
    column = lax.broadcasted_iota(jnp.int32, (tokens, tokens), 1)
    before = jnp.where(column < row, 1.0, 0.0).astype(jnp.bfloat16)
    rank = dot(before, member.astype(jnp.bfloat16))
    slot = (lane % capacity).astype(jnp.float32)
    place = jnp.where(rank == slot, member, 0.0)
    mix = place * weight
    row = lax.broadcasted_iota(jnp.int32, (wide, wide), 0)
    column = lax.broadcasted_iota(jnp.int32, (wide, wide), 1)
    eye = jnp.where(column == row, 1.0, 0.0).astype(jnp.bfloat16)
    pick = lax.dot_general(
        eye,
        place.astype(jnp.bfloat16),
        (((1,), (1,)), ((), ())),
        preferred_element_type=jnp.float32,
    )
    return pick.astype(jnp.bfloat16), mix


def kernel(
    groups, experts, tokens, ids, codes, w_gate, w_up, w_down, out,
    tok, ids_v, codes_v, wg, wu, wd, rows, slots, part, ret, mixed, red,
    in_sem, w_sem, ga_s, ga_r, di_s, di_r, re_s, re_r, sc_s, sc_r,
):
    g = lax.axis_index("group")
    z = lax.axis_index("expert")
    own = tokens.shape[0]
    width = tokens.shape[1]
    size = width // CHUNKS
    cuts = [pl.ds(c * size, size) for c in range(CHUNKS)]
    cap = CAPG

    tok_in = pltpu.make_async_copy(tokens, tok.at[g], in_sem.at[0])
    ids_in = pltpu.make_async_copy(ids, ids_v, in_sem.at[1])
    codes_in = pltpu.make_async_copy(codes, codes_v, in_sem.at[2])
    tok_in.start()
    ids_in.start()
    codes_in.start()

    barrier = pltpu.get_barrier_semaphore()
    group_peers = [lax.rem(g + k, groups) for k in range(1, groups)]
    expert_peers = [lax.rem(z + k, experts) for k in range(1, experts)]
    for peer in group_peers:
        pl.semaphore_signal(barrier, inc=1, device_id={"group": peer}, device_id_type=MESH)
    for peer in expert_peers:
        pl.semaphore_signal(barrier, inc=1, device_id={"expert": peer}, device_id_type=MESH)

    gate_in = [pltpu.make_async_copy(w_gate.at[cut, :], wg.at[cut, :], w_sem.at[0, c]) for c, cut in enumerate(cuts)]
    up_in = [pltpu.make_async_copy(w_up.at[cut, :], wu.at[cut, :], w_sem.at[1, c]) for c, cut in enumerate(cuts)]
    down_in = [pltpu.make_async_copy(w_down.at[:, cut], wd.at[:, cut], w_sem.at[2, c]) for c, cut in enumerate(cuts)]
    for c in range(CHUNKS):
        gate_in[c].start()
        up_in[c].start()
    for c in range(CHUNKS):
        down_in[c].start()

    ids_in.wait()
    codes_in.wait()
    pick, mix = routing(ids_v[...], codes_v[...], experts, cap)
    mix_hi = mix.astype(jnp.bfloat16)
    mix_lo = (mix - mix_hi.astype(jnp.float32)).astype(jnp.bfloat16)
    tok_in.wait()
    pl.semaphore_wait(barrier, groups + experts - 2)

    def remote(axis, peer, src, dst, send, recv):
        return pltpu.make_async_remote_copy(
            src_ref=src, dst_ref=dst, send_sem=send, recv_sem=recv,
            device_id={axis: peer}, device_id_type=MESH,
        )

    gather = [
        [
            remote("group", peer, tok.at[g, :, cut], tok.at[g, :, cut], ga_s.at[c, k], ga_r.at[c, k])
            for k, peer in enumerate(group_peers)
        ]
        for c, cut in enumerate(cuts)
    ]
    dispatch = [
        [
            remote("expert", peer, rows.at[peer, :, cut], slots.at[z, :, cut], di_s.at[c, k], di_r.at[c, k])
            for k, peer in enumerate(expert_peers)
        ]
        for c, cut in enumerate(cuts)
    ]
    giveback = [
        [
            remote("expert", peer, part.at[peer, :, cut], ret.at[z, :, cut], re_s.at[c, k], re_r.at[c, k])
            for k, peer in enumerate(expert_peers)
        ]
        for c, cut in enumerate(cuts)
    ]
    scatter = [
        [
            remote("group", peer, mixed.at[peer, :, cut], red.at[g, :, cut], sc_s.at[c, k], sc_r.at[c, k])
            for k, peer in enumerate(group_peers)
        ]
        for c, cut in enumerate(cuts)
    ]

    for c in range(CHUNKS):
        for copy in gather[c]:
            copy.start()
    for c, cut in enumerate(cuts):
        for copy in gather[c]:
            copy.wait_recv()
        chosen = dot(pick, tok[:, :, cut].reshape(groups * own, size)).astype(jnp.bfloat16)
        rows[:, :, cut] = chosen.reshape(experts, cap, size)
        for copy in dispatch[c]:
            copy.start()
        slots[z, :, cut] = rows[z, :, cut]

    first = second = None
    for c, cut in enumerate(cuts):
        for copy in dispatch[c]:
            copy.wait_recv()
        gate_in[c].wait()
        up_in[c].wait()
        flat = slots[:, :, cut].reshape(experts * cap, size)
        a = dot(flat, wg[cut, :])
        b = dot(flat, wu[cut, :])
        first = a if first is None else first + a
        second = b if second is None else second + b
    hidden = (first / (1.0 + jnp.exp(-first)) * second).astype(jnp.bfloat16)

    for c, cut in enumerate(cuts):
        down_in[c].wait()
        made = dot(hidden, wd[:, cut]).astype(jnp.bfloat16)
        part[:, :, cut] = made.reshape(experts, cap, size)
        for copy in giveback[c]:
            copy.start()
        ret[z, :, cut] = part[z, :, cut]

    for c, cut in enumerate(cuts):
        for copy in giveback[c]:
            copy.wait_recv()
        back = ret[:, :, cut].reshape(experts * cap, size)
        total = (dot(mix_hi, back) + dot(mix_lo, back)).astype(jnp.bfloat16)
        mixed[:, :, cut] = total.reshape(groups, own, size)
        for copy in scatter[c]:
            copy.start()
        red[g, :, cut] = mixed[g, :, cut]

    for c, cut in enumerate(cuts):
        for copy in scatter[c]:
            copy.wait_recv()
        out[:, cut] = jnp.sum(red[:, :, cut].astype(jnp.float32), axis=0).astype(jnp.bfloat16)

    for phase in (gather, dispatch, giveback, scatter):
        for copies in phase:
            for copy in copies:
                copy.wait_send()


def per_device(tokens, expert_ids, gate_codes, w_gate, w_up, w_down):
    groups = lax.axis_size("group")
    experts = lax.axis_size("expert")
    own, width = tokens.shape[1:]
    hid = w_gate.shape[2]
    bf16 = jnp.bfloat16
    any_space = pl.BlockSpec(memory_space=pl.ANY)
    dma = pltpu.SemaphoreType.DMA
    mixed = pl.pallas_call(
        functools.partial(kernel, groups, experts),
        out_shape=jax.ShapeDtypeStruct((own, width), bf16),
        in_specs=[any_space] * 6,
        out_specs=pl.BlockSpec(memory_space=pltpu.VMEM),
        scratch_shapes=[
            pltpu.VMEM((groups, own, width), bf16),
            pltpu.VMEM(expert_ids.shape[1:], jnp.int32),
            pltpu.VMEM(gate_codes.shape[1:], jnp.int32),
            pltpu.VMEM((width, hid), bf16),
            pltpu.VMEM((width, hid), bf16),
            pltpu.VMEM((hid, width), bf16),
            pltpu.VMEM((experts, CAPG, width), bf16),
            pltpu.VMEM((experts, CAPG, width), bf16),
            pltpu.VMEM((experts, CAPG, width), bf16),
            pltpu.VMEM((experts, CAPG, width), bf16),
            pltpu.VMEM((groups, own, width), bf16),
            pltpu.VMEM((groups, own, width), bf16),
            dma((3,)),
            dma((3, CHUNKS)),
            dma((CHUNKS, groups - 1)),
            dma((CHUNKS, groups - 1)),
            dma((CHUNKS, experts - 1)),
            dma((CHUNKS, experts - 1)),
            dma((CHUNKS, experts - 1)),
            dma((CHUNKS, experts - 1)),
            dma((CHUNKS, groups - 1)),
            dma((CHUNKS, groups - 1)),
        ],
        compiler_params=pltpu.CompilerParams(
            collective_id=0, has_side_effects=True, vmem_limit_bytes=60 * 1024 * 1024
        ),
    )(tokens[0], expert_ids[0], gate_codes[0], w_gate[0], w_up[0], w_down[0])
    return mixed[None]


def solution(mesh):
    placed = (
        P(("expert", "dp"), "group", None),
        P(("expert", "dp"), None, None),
        P(("expert", "dp"), None, None),
        P("expert", None, "group"),
        P("expert", None, "group"),
        P("expert", "group", None),
    )
    return jax.shard_map(
        per_device,
        mesh=mesh,
        in_specs=placed,
        out_specs=P(("expert", "dp"), "group", None),
        check_vma=False,
    )
```

```python
import functools

import jax
import jax.numpy as jnp
from jax import lax
from jax.experimental import pallas as pl
from jax.experimental.pallas import tpu as pltpu
from jax.sharding import PartitionSpec as P

CAPG = 4
FORWARD = (1, 1, 1, 1)
BACK = (1, 1, 1, 1)
MESH = pl.DeviceIdType.MESH


def dot(a, b):
    return jnp.dot(a, b, preferred_element_type=jnp.float32)


def routing(ids, codes, experts, capacity):
    tokens = ids.shape[1]
    wide = experts * capacity
    codes = codes.astype(jnp.float32)
    gates = 2.5 * codes / jnp.sum(codes, axis=0, keepdims=True)
    slot = lax.broadcasted_iota(jnp.int32, (wide, tokens), 0)
    member = jnp.zeros((wide, tokens), jnp.float32)
    weight = jnp.zeros((wide, tokens), jnp.float32)
    for e in range(experts):
        hits = ids == e
        named = jnp.max(jnp.where(hits, 1.0, 0.0), axis=0, keepdims=True)
        gate = jnp.sum(jnp.where(hits, gates, 0.0), axis=0, keepdims=True)
        mine = (slot >= e * capacity) & (slot < (e + 1) * capacity)
        member = jnp.where(mine, named, member)
        weight = jnp.where(mine, gate, weight)
    row = lax.broadcasted_iota(jnp.int32, (tokens, tokens), 0)
    column = lax.broadcasted_iota(jnp.int32, (tokens, tokens), 1)
    before = jnp.where(row < column, 1.0, 0.0).astype(jnp.bfloat16)
    rank = dot(member.astype(jnp.bfloat16), before)
    place = jnp.where(rank == (slot % capacity).astype(jnp.float32), member, 0.0)
    return place, place * weight


def flipped(a):
    n = a.shape[1]
    row = lax.broadcasted_iota(jnp.int32, (n, n), 0)
    column = lax.broadcasted_iota(jnp.int32, (n, n), 1)
    eye = jnp.where(row == column, 1.0, 0.0).astype(jnp.bfloat16)
    return lax.dot_general(
        eye, a, (((1,), (1,)), ((), ())), preferred_element_type=jnp.float32
    ).astype(jnp.bfloat16)


def pieces(width, shares):
    ends = [0]
    for k in range(len(shares)):
        ends.append(width * sum(shares[: k + 1]) // sum(shares) // 128 * 128)
    return [pl.ds(a, b - a) for a, b in zip(ends[:-1], ends[1:])]


def kernel(
    groups, experts, tokens, ids, codes, w_gate, w_up, w_down, red,
    tok, ids_v, codes_v, wg, wu, wd, rows, slots, part, ret, mixed,
    in_sem, w_sem, d_sem, ga_s, ga_r, di_s, di_r, re_s, re_r, sc_s, sc_r, k_sem,
):
    g = lax.axis_index("group")
    z = lax.axis_index("expert")
    own = tokens.shape[0]
    width = tokens.shape[1]
    cuts = pieces(width, FORWARD)
    back_cuts = pieces(width, BACK)
    cap = CAPG

    tok_in = pltpu.make_async_copy(tokens, tok.at[g], in_sem.at[0])
    ids_in = pltpu.make_async_copy(ids, ids_v, in_sem.at[1])
    codes_in = pltpu.make_async_copy(codes, codes_v, in_sem.at[2])
    tok_in.start()
    ids_in.start()
    codes_in.start()

    barrier = pltpu.get_barrier_semaphore()
    group_peers = [lax.rem(g + k, groups) for k in range(1, groups)]
    expert_peers = [lax.rem(z + k, experts) for k in range(1, experts)]
    for peer in group_peers:
        pl.semaphore_signal(barrier, inc=1, device_id={"group": peer}, device_id_type=MESH)
    for peer in expert_peers:
        pl.semaphore_signal(barrier, inc=1, device_id={"expert": peer}, device_id_type=MESH)

    gate_in = [pltpu.make_async_copy(w_gate.at[cut, :], wg.at[cut, :], w_sem.at[0, c]) for c, cut in enumerate(cuts)]
    up_in = [pltpu.make_async_copy(w_up.at[cut, :], wu.at[cut, :], w_sem.at[1, c]) for c, cut in enumerate(cuts)]
    down_in = [pltpu.make_async_copy(w_down.at[:, cut], wd.at[:, cut], d_sem.at[c]) for c, cut in enumerate(back_cuts)]
    for c in range(len(cuts)):
        gate_in[c].start()
        up_in[c].start()
    for c in range(len(back_cuts)):
        down_in[c].start()

    ids_in.wait()
    codes_in.wait()
    pick, mix = routing(ids_v[...], codes_v[...], experts, cap)
    pick = pick.astype(jnp.bfloat16)
    mix_hi = mix.astype(jnp.bfloat16)
    mix_lo = flipped((mix - mix_hi.astype(jnp.float32)).astype(jnp.bfloat16))
    mix_hi = flipped(mix_hi)
    tok_in.wait()
    pl.semaphore_wait(barrier, groups + experts - 2)

    def remote(axis, peer, src, dst, send, recv):
        return pltpu.make_async_remote_copy(
            src_ref=src, dst_ref=dst, send_sem=send, recv_sem=recv,
            device_id={axis: peer}, device_id_type=MESH,
        )

    gather = [
        [
            remote("group", peer, tok.at[g, :, cut], tok.at[g, :, cut], ga_s.at[c, k], ga_r.at[c, k])
            for k, peer in enumerate(group_peers)
        ]
        for c, cut in enumerate(cuts)
    ]
    dispatch = [
        [
            remote("expert", peer, rows.at[peer, :, cut], slots.at[z, :, cut], di_s.at[c, k], di_r.at[c, k])
            for k, peer in enumerate(expert_peers)
        ]
        for c, cut in enumerate(cuts)
    ]
    giveback = [
        [
            remote("expert", peer, part.at[peer, :, cut], ret.at[z, :, cut], re_s.at[c, k], re_r.at[c, k])
            for k, peer in enumerate(expert_peers)
        ]
        for c, cut in enumerate(back_cuts)
    ]
    scatter = [
        [
            remote("group", peer, mixed.at[peer, :, cut], red.at[g, :, cut], sc_s.at[c, k], sc_r.at[c, k])
            for k, peer in enumerate(group_peers)
        ]
        for c, cut in enumerate(back_cuts)
    ]

    for c in range(len(cuts)):
        for copy in gather[c]:
            copy.start()
    for c, cut in enumerate(cuts):
        for copy in gather[c]:
            copy.wait_recv()
        chosen = dot(pick, tok[:, :, cut].reshape(groups * own, cut.size)).astype(jnp.bfloat16)
        rows[:, :, cut] = chosen.reshape(experts, cap, cut.size)
        for copy in dispatch[c]:
            copy.start()
        slots[z, :, cut] = rows[z, :, cut]

    first = second = None
    for c, cut in enumerate(cuts):
        for copy in dispatch[c]:
            copy.wait_recv()
        gate_in[c].wait()
        up_in[c].wait()
        flat = slots[:, :, cut].reshape(experts * cap, cut.size)
        a = dot(flat, wg[cut, :])
        b = dot(flat, wu[cut, :])
        first = a if first is None else first + a
        second = b if second is None else second + b
    hidden = (first / (1.0 + jnp.exp(-first)) * second).astype(jnp.bfloat16)

    for c, cut in enumerate(back_cuts):
        down_in[c].wait()
        made = dot(hidden, wd[:, cut]).astype(jnp.bfloat16)
        part[:, :, cut] = made.reshape(experts, cap, cut.size)
        for copy in giveback[c]:
            copy.start()
        ret[z, :, cut] = part[z, :, cut]

    keep = []
    for c, cut in enumerate(back_cuts):
        for copy in giveback[c]:
            copy.wait_recv()
        back = ret[:, :, cut].reshape(experts * cap, cut.size)
        total = (dot(mix_hi, back) + dot(mix_lo, back)).astype(jnp.bfloat16)
        mixed[:, :, cut] = total.reshape(groups, own, cut.size)
        for copy in scatter[c]:
            copy.start()
        keep.append(pltpu.make_async_copy(mixed.at[g, :, cut], red.at[g, :, cut], k_sem.at[c]))
        keep[c].start()

    for c in range(len(back_cuts)):
        for copy in scatter[c]:
            copy.wait_recv()
        keep[c].wait()

    for phase in (gather, dispatch, giveback, scatter):
        for copies in phase:
            for copy in copies:
                copy.wait_send()


def per_device(tokens, expert_ids, gate_codes, w_gate, w_up, w_down):
    groups = lax.axis_size("group")
    experts = lax.axis_size("expert")
    own, width = tokens.shape[1:]
    hid = w_gate.shape[2]
    bf16 = jnp.bfloat16
    any_space = pl.BlockSpec(memory_space=pl.ANY)
    dma = pltpu.SemaphoreType.DMA
    shares = pl.pallas_call(
        functools.partial(kernel, groups, experts),
        out_shape=jax.ShapeDtypeStruct((groups, own, width), bf16),
        in_specs=[any_space] * 6,
        out_specs=any_space,
        scratch_shapes=[
            pltpu.VMEM((groups, own, width), bf16),
            pltpu.VMEM(expert_ids.shape[:0:-1], jnp.int32),
            pltpu.VMEM(gate_codes.shape[:0:-1], jnp.int32),
            pltpu.VMEM((width, hid), bf16),
            pltpu.VMEM((width, hid), bf16),
            pltpu.VMEM((hid, width), bf16),
            pltpu.VMEM((experts, CAPG, width), bf16),
            pltpu.VMEM((experts, CAPG, width), bf16),
            pltpu.VMEM((experts, CAPG, width), bf16),
            pltpu.VMEM((experts, CAPG, width), bf16),
            pltpu.VMEM((groups, own, width), bf16),
            dma((3,)),
            dma((2, len(FORWARD))),
            dma((len(BACK),)),
            dma((len(FORWARD), groups - 1)),
            dma((len(FORWARD), groups - 1)),
            dma((len(FORWARD), experts - 1)),
            dma((len(FORWARD), experts - 1)),
            dma((len(BACK), experts - 1)),
            dma((len(BACK), experts - 1)),
            dma((len(BACK), groups - 1)),
            dma((len(BACK), groups - 1)),
            dma((len(BACK),)),
        ],
        compiler_params=pltpu.CompilerParams(
            collective_id=0, has_side_effects=True, vmem_limit_bytes=60 * 1024 * 1024
        ),
    )(tokens[0], expert_ids[0].T, gate_codes[0].T, w_gate[0], w_up[0], w_down[0])
    total = shares[0].astype(jnp.float32)
    for k in range(1, groups):
        total = total + shares[k].astype(jnp.float32)
    return total.astype(bf16)[None]


def solution(mesh):
    placed = (
        P(("expert", "dp"), "group", None),
        P(("expert", "dp"), None, None),
        P(("expert", "dp"), None, None),
        P("expert", None, "group"),
        P("expert", None, "group"),
        P("expert", "group", None),
    )
    return jax.shard_map(
        per_device,
        mesh=mesh,
        in_specs=placed,
        out_specs=P(("expert", "dp"), "group", None),
        check_vma=False,
    )
```

```python
import functools

import jax
import jax.numpy as jnp
from jax import lax
from jax.experimental import pallas as pl
from jax.experimental.pallas import tpu as pltpu
from jax.sharding import PartitionSpec as P

CAPG = 4
GATHER = (1, 1, 1, 1)
FORWARD = (1, 1, 1, 1)
BACK = (1, 1, 1, 1)
MESH = pl.DeviceIdType.MESH


def dot(a, b):
    return jnp.dot(a, b, preferred_element_type=jnp.float32)


def routing(ids, codes, experts, capacity):
    tokens = ids.shape[1]
    wide = experts * capacity
    codes = codes.astype(jnp.float32)
    gates = 2.5 * codes / jnp.sum(codes, axis=0, keepdims=True)
    slot = lax.broadcasted_iota(jnp.int32, (wide, tokens), 0)
    member = jnp.zeros((wide, tokens), jnp.float32)
    weight = jnp.zeros((wide, tokens), jnp.float32)
    for e in range(experts):
        hits = ids == e
        named = jnp.max(jnp.where(hits, 1.0, 0.0), axis=0, keepdims=True)
        gate = jnp.sum(jnp.where(hits, gates, 0.0), axis=0, keepdims=True)
        mine = (slot >= e * capacity) & (slot < (e + 1) * capacity)
        member = jnp.where(mine, named, member)
        weight = jnp.where(mine, gate, weight)
    row = lax.broadcasted_iota(jnp.int32, (tokens, tokens), 0)
    column = lax.broadcasted_iota(jnp.int32, (tokens, tokens), 1)
    before = jnp.where(row < column, 1.0, 0.0).astype(jnp.bfloat16)
    rank = dot(member.astype(jnp.bfloat16), before)
    place = jnp.where(rank == (slot % capacity).astype(jnp.float32), member, 0.0)
    return place, place * weight


def flipped(a):
    n = a.shape[1]
    row = lax.broadcasted_iota(jnp.int32, (n, n), 0)
    column = lax.broadcasted_iota(jnp.int32, (n, n), 1)
    eye = jnp.where(row == column, 1.0, 0.0).astype(jnp.bfloat16)
    return lax.dot_general(
        eye, a, (((1,), (1,)), ((), ())), preferred_element_type=jnp.float32
    ).astype(jnp.bfloat16)


def pieces(width, shares):
    ends = [0]
    for k in range(len(shares)):
        ends.append(width * sum(shares[: k + 1]) // sum(shares) // 128 * 128)
    return [pl.ds(a, b - a) for a, b in zip(ends[:-1], ends[1:])]


def partners(me, count):
    found = []
    for k in range(count - 1, 0, -1):
        peer, bit = 0, 1
        while bit < count:
            peer += lax.rem(me // bit + k // bit, 2) * bit
            bit *= 2
        found.append(peer)
    return found


def kernel(
    groups, experts, tokens, ids, codes, w_gate, w_up, w_down, red,
    tok, ids_v, codes_v, wg, wu, wd, rows, slots, part, ret, mixed,
    in_sem, w_sem, d_sem, ga_s, ga_r, di_s, di_r, re_s, re_r, sc_s, sc_r, k_sem,
):
    g = lax.axis_index("group")
    z = lax.axis_index("expert")
    own = tokens.shape[0]
    width = tokens.shape[1]
    wide_cuts = pieces(width, GATHER)
    cuts = pieces(width, FORWARD)
    back_cuts = pieces(width, BACK)
    cap = CAPG

    tok_in = pltpu.make_async_copy(tokens, tok.at[g], in_sem.at[0])
    ids_in = pltpu.make_async_copy(ids, ids_v, in_sem.at[1])
    codes_in = pltpu.make_async_copy(codes, codes_v, in_sem.at[2])
    tok_in.start()
    ids_in.start()
    codes_in.start()

    barrier = pltpu.get_barrier_semaphore()
    group_peers = partners(g, groups)
    expert_peers = [lax.rem(z + k, experts) for k in range(1, experts)]
    for peer in group_peers:
        pl.semaphore_signal(barrier, inc=1, device_id={"group": peer}, device_id_type=MESH)
    for peer in expert_peers:
        pl.semaphore_signal(barrier, inc=1, device_id={"expert": peer}, device_id_type=MESH)

    gate_in = [pltpu.make_async_copy(w_gate.at[cut, :], wg.at[cut, :], w_sem.at[0, c]) for c, cut in enumerate(cuts)]
    up_in = [pltpu.make_async_copy(w_up.at[cut, :], wu.at[cut, :], w_sem.at[1, c]) for c, cut in enumerate(cuts)]
    down_in = [pltpu.make_async_copy(w_down.at[:, cut], wd.at[:, cut], d_sem.at[c]) for c, cut in enumerate(back_cuts)]
    ids_in.wait()
    codes_in.wait()
    tok_in.wait()
    for c in range(len(cuts)):
        gate_in[c].start()
        up_in[c].start()
    for c in range(len(back_cuts)):
        down_in[c].start()

    pick, mix = routing(ids_v[...], codes_v[...], experts, cap)
    pick = pick.astype(jnp.bfloat16)
    mix_hi = mix.astype(jnp.bfloat16)
    mix_lo = flipped((mix - mix_hi.astype(jnp.float32)).astype(jnp.bfloat16))
    mix_hi = flipped(mix_hi)
    pl.semaphore_wait(barrier, groups + experts - 2)

    def remote(axis, peer, src, dst, send, recv):
        return pltpu.make_async_remote_copy(
            src_ref=src, dst_ref=dst, send_sem=send, recv_sem=recv,
            device_id={axis: peer}, device_id_type=MESH,
        )

    gather = [
        [
            remote("group", peer, tok.at[g, :, cut], tok.at[g, :, cut], ga_s.at[c, k], ga_r.at[c, k])
            for k, peer in enumerate(group_peers)
        ]
        for c, cut in enumerate(wide_cuts)
    ]
    dispatch = [
        [
            remote("expert", peer, rows.at[peer, :, cut], slots.at[z, :, cut], di_s.at[c, k], di_r.at[c, k])
            for k, peer in enumerate(expert_peers)
        ]
        for c, cut in enumerate(cuts)
    ]
    giveback = [
        [
            remote("expert", peer, part.at[peer, :, cut], ret.at[z, :, cut], re_s.at[c, k], re_r.at[c, k])
            for k, peer in enumerate(expert_peers)
        ]
        for c, cut in enumerate(back_cuts)
    ]
    scatter = [
        [
            remote("group", peer, mixed.at[peer, :, cut], red.at[g, :, cut], sc_s.at[c, k], sc_r.at[c, k])
            for k, peer in enumerate(group_peers)
        ]
        for c, cut in enumerate(back_cuts)
    ]

    for copies in gather:
        for copy in copies:
            copy.start()
    here = 0
    for c, cut in enumerate(cuts):
        while here < len(wide_cuts) and wide_cuts[here].start < cut.start + cut.size:
            for copy in gather[here]:
                copy.wait_recv()
            here += 1
        chosen = dot(pick, tok[:, :, cut].reshape(groups * own, cut.size)).astype(jnp.bfloat16)
        rows[:, :, cut] = chosen.reshape(experts, cap, cut.size)
        for copy in dispatch[c]:
            copy.start()
        slots[z, :, cut] = rows[z, :, cut]

    first = second = None
    for c, cut in enumerate(cuts):
        for copy in dispatch[c]:
            copy.wait_recv()
        gate_in[c].wait()
        up_in[c].wait()
        flat = slots[:, :, cut].reshape(experts * cap, cut.size)
        a = dot(flat, wg[cut, :])
        b = dot(flat, wu[cut, :])
        first = a if first is None else first + a
        second = b if second is None else second + b
    hidden = (first / (1.0 + jnp.exp(-first)) * second).astype(jnp.bfloat16)

    for c, cut in enumerate(back_cuts):
        down_in[c].wait()
        made = dot(hidden, wd[:, cut]).astype(jnp.bfloat16)
        part[:, :, cut] = made.reshape(experts, cap, cut.size)
        for copy in giveback[c]:
            copy.start()
        ret[z, :, cut] = part[z, :, cut]

    keep = []
    for c, cut in enumerate(back_cuts):
        for copy in giveback[c]:
            copy.wait_recv()
        back = ret[:, :, cut].reshape(experts * cap, cut.size)
        total = (dot(mix_hi, back) + dot(mix_lo, back)).astype(jnp.bfloat16)
        mixed[:, :, cut] = total.reshape(groups, own, cut.size)
        for copy in scatter[c]:
            copy.start()
        keep.append(pltpu.make_async_copy(mixed.at[g, :, cut], red.at[g, :, cut], k_sem.at[c]))
        keep[c].start()

    for c in range(len(back_cuts)):
        for copy in scatter[c]:
            copy.wait_recv()
        keep[c].wait()

    for phase in (gather, dispatch, giveback, scatter):
        for copies in phase:
            for copy in copies:
                copy.wait_send()


def per_device(tokens, expert_ids, gate_codes, w_gate, w_up, w_down):
    groups = lax.axis_size("group")
    experts = lax.axis_size("expert")
    own, width = tokens.shape[1:]
    hid = w_gate.shape[2]
    bf16 = jnp.bfloat16
    any_space = pl.BlockSpec(memory_space=pl.ANY)
    dma = pltpu.SemaphoreType.DMA
    shares = pl.pallas_call(
        functools.partial(kernel, groups, experts),
        out_shape=jax.ShapeDtypeStruct((groups, own, width), bf16),
        in_specs=[any_space] * 6,
        out_specs=any_space,
        scratch_shapes=[
            pltpu.VMEM((groups, own, width), bf16),
            pltpu.VMEM(expert_ids.shape[:0:-1], jnp.int32),
            pltpu.VMEM(gate_codes.shape[:0:-1], jnp.int32),
            pltpu.VMEM((width, hid), bf16),
            pltpu.VMEM((width, hid), bf16),
            pltpu.VMEM((hid, width), bf16),
            pltpu.VMEM((experts, CAPG, width), bf16),
            pltpu.VMEM((experts, CAPG, width), bf16),
            pltpu.VMEM((experts, CAPG, width), bf16),
            pltpu.VMEM((experts, CAPG, width), bf16),
            pltpu.VMEM((groups, own, width), bf16),
            dma((3,)),
            dma((2, len(FORWARD))),
            dma((len(BACK),)),
            dma((len(GATHER), groups - 1)),
            dma((len(GATHER), groups - 1)),
            dma((len(FORWARD), experts - 1)),
            dma((len(FORWARD), experts - 1)),
            dma((len(BACK), experts - 1)),
            dma((len(BACK), experts - 1)),
            dma((len(BACK), groups - 1)),
            dma((len(BACK), groups - 1)),
            dma((len(BACK),)),
        ],
        compiler_params=pltpu.CompilerParams(
            collective_id=0, has_side_effects=True, vmem_limit_bytes=60 * 1024 * 1024
        ),
    )(tokens[0], expert_ids[0].T, gate_codes[0].T, w_gate[0], w_up[0], w_down[0])
    total = shares[0].astype(jnp.float32)
    for k in range(1, groups):
        total = total + shares[k].astype(jnp.float32)
    return total.astype(bf16)[None]


def solution(mesh):
    placed = (
        P(("expert", "dp"), "group", None),
        P(("expert", "dp"), None, None),
        P(("expert", "dp"), None, None),
        P("expert", None, "group"),
        P("expert", None, "group"),
        P("expert", "group", None),
    )
    return jax.shard_map(
        per_device,
        mesh=mesh,
        in_specs=placed,
        out_specs=P(("expert", "dp"), "group", None),
        check_vma=False,
    )
```
